32 devices in a mesh: rep: 1, dp: 32 (over x, y, z, core).
Axes of the slice: x: 2, y: 2, z: 4, core: 2. Of those that a mesh axis runs over, the one named last changes fastest.
Arguments:
- x: bfloat16 [32, 2048, 896], P(('rep', 'dp'))
- dy: bfloat16 [32, 2048, 896], P(('rep', 'dp'))
- w_gate: bfloat16 [2, 896, 2560], replicated
- w_up: bfloat16 [2, 896, 2560], replicated
- w_down: bfloat16 [2, 2560, 896], replicated
- m_w_gate: float32 [2, 896, 2560], replicated
- m_w_up: float32 [2, 896, 2560], replicated
- m_w_down: float32 [2, 2560, 896], replicated
- v_w_gate: float32 [2, 896, 2560], replicated
- v_w_up: float32 [2, 896, 2560], replicated
- v_w_down: float32 [2, 2560, 896], replicated
Outputs:
- output 1: bfloat16 [2, 896, 2560], P('rep')
- output 2: bfloat16 [2, 896, 2560], P('rep')
- output 3: bfloat16 [2, 2560, 896], P('rep')
- output 4: float32 [2, 896, 2560], P('rep')
- output 5: float32 [2, 896, 2560], P('rep')
- output 6: float32 [2, 2560, 896], P('rep')
- output 7: float32 [2, 896, 2560], P('rep')
- output 8: float32 [2, 896, 2560], P('rep')
- output 9: float32 [2, 2560, 896], P('rep')
All inputs are finite; a program needn't handle non-finite values.
Results may differ from the reference program's by a relative error of at most 0.022.
Values are sent between devices in bfloat16 or wider.
A program may use at most 2.5 GiB of HBM per device.

```python
import jax
import jax.numpy as jnp
from jax import lax

SEQUENCES = 32
TOKENS = 2048
D = 896
FF = 2560
LAYERS = 2
NAMES = ("w_gate", "w_up", "w_down")
SHAPES = {"w_gate": (LAYERS, D, FF), "w_up": (LAYERS, D, FF), "w_down": (LAYERS, FF, D)}


def bump(key, n, height):
    away = (jnp.arange(n, dtype=jnp.int32) - jax.random.randint(key, (), 0, n, jnp.int32)) % n
    return jnp.where(away < n // 8, height, 1.0)


def together(key, own, strength):
    shared = jax.random.normal(key, own.shape[1:], jnp.float32)
    return (own + strength * shared) * lax.rsqrt(1 + strength * strength)


def setup_inputs(seed: int = 0, part: int = 0) -> dict:
    kx, kdy, ka, kb, kz, kf, kh, kl, *keys = jax.random.split(jax.random.key(seed), 8 + 3 * len(NAMES))
    kx, kdy, ka, kb = (jax.random.fold_in(k, part) for k in (kx, kdy, ka, kb))
    kw, km, kv = (keys[i::3] for i in range(3))
    shape = (SEQUENCES, TOKENS, D)
    much_x, much_dy = jax.random.uniform(kz, (2,), jnp.float32, 0.0, 1.0)
    loud = 2.0 ** jax.random.uniform(jax.random.fold_in(kz, 1), (), jnp.float32, -1.0, 2.0)
    layers = 2.0 ** jax.random.uniform(kl, (LAYERS, 1, 1), jnp.float32, -1.0, 1.0)
    x = together(ka, jax.random.normal(kx, shape, jnp.float32), much_x) * bump(kf, D, 4.0)
    dy = together(kb, jax.random.normal(kdy, shape, jnp.float32), much_dy)
    drawn = {"x": x.astype(jnp.bfloat16), "dy": (loud * dy * (SEQUENCES * TOKENS) ** -0.5).astype(jnp.bfloat16)}
    for key, name in zip(kw, NAMES, strict=True):
        w = jax.random.normal(key, SHAPES[name], jnp.float32) * SHAPES[name][1] ** -0.5
        drawn[name] = (w * {"w_gate": 1.0, "w_up": bump(kh, FF, 4.0), "w_down": layers}[name]).astype(jnp.bfloat16)
    for key, name in zip(km, NAMES, strict=True):
        drawn[f"m_{name}"] = 0.1 * jax.random.normal(key, SHAPES[name], jnp.float32)
    for key, name in zip(kv, NAMES, strict=True):
        drawn[f"v_{name}"] = jax.random.uniform(key, SHAPES[name], jnp.float32, 0.005, 0.015)
    return drawn


def matmul(a, w):
    return jnp.dot(a, w, preferred_element_type=jnp.float32).astype(jnp.bfloat16)


def normed(h):
    wide = h.astype(jnp.float32)
    scale = lax.rsqrt(jnp.mean(wide**2, -1, keepdims=True) + 1e-6)
    return (wide * scale).astype(jnp.bfloat16)


def layer(h, w):
    a = normed(h)
    gate = jnp.dot(a, w["w_gate"], preferred_element_type=jnp.float32)
    up = jnp.dot(a, w["w_up"], preferred_element_type=jnp.float32)
    return h + matmul((jax.nn.silu(gate) * up).astype(jnp.bfloat16), w["w_down"])


def adamw(w, m, v, g):
    m = 0.9 * m + 0.1 * g
    v = 0.95 * v + 0.05 * g * g
    step = m * lax.rsqrt(v + 1e-8) + 0.1 * w
    return (w - 0.02 * step).astype(jnp.bfloat16), m, v


def clipped(gradients, sum_of_squares, count):
    factor = jnp.minimum(1.0, 0.5 * lax.rsqrt(sum_of_squares / count + 1e-30))
    return [g * factor for g in gradients]


def stack(weights, h):
    return lax.scan(lambda h, w: (layer(h, w), None), h, weights)[0]


def reference(x, dy, w_gate, w_up, w_down, m_w_gate, m_w_up, m_w_down, v_w_gate, v_w_up, v_w_down):
    weights = dict(zip(NAMES, (w_gate, w_up, w_down), strict=True))

    def take(so_far, sequence):
        h, by_y = sequence
        _, back = jax.vjp(lambda w: stack(w, h), weights)
        return jax.tree.map(lambda total, term: total + term.astype(jnp.float32), so_far, back(by_y)[0]), None

    none_yet = {name: jnp.zeros(w.shape, jnp.float32) for name, w in weights.items()}
    by_weights, _ = lax.scan(take, none_yet, (x, dy))
    gradients = [by_weights[name].astype(jnp.bfloat16).astype(jnp.float32) for name in NAMES]
    gradients = clipped(gradients, sum(jnp.sum(g * g) for g in gradients), sum(g.size for g in gradients))
    new = [
        adamw(w.astype(jnp.float32), m, v, g)
        for w, m, v, g in zip((w_gate, w_up, w_down), (m_w_gate, m_w_up, m_w_down), (v_w_gate, v_w_up, v_w_down), gradients, strict=True)
    ]
    return tuple(one[which] for which in range(3) for one in new)
```

```python
import functools

import jax
import jax.numpy as jnp
from jax import lax
from jax.experimental import pallas as pl
from jax.experimental.pallas import tpu as pltpu
from jax.sharding import PartitionSpec as P

NAMES = ("w_gate", "w_up", "w_down")
DEVICES = 32
CORE, Z1, Z2, Y, X = 1, 2, 4, 8, 16
XY = {0: (X, Y), 1: (Y, X)}


BLOCK = 256
CHUNK = 512


def dot(a, b):
    return jnp.dot(a, b, preferred_element_type=jnp.float32)


def narrow(a):
    return a.astype(jnp.bfloat16)


def normed(h):
    wide = h.astype(jnp.float32)
    return narrow(wide * lax.rsqrt(jnp.mean(wide**2, -1, keepdims=True) + 1e-6))


def turned(source, target):
    def some(i, _):
        at = pl.ds(pl.multiple_of(i * 128, 128), 128)
        target[:, at] = source[at, :].T
        return 0

    lax.fori_loop(0, source.shape[0] // 128, some, 0)


def first_kernel(x_ref, dy_ref, wg_any, wu_any, wd_any, a1_ref, g1_ref, u1_ref, hid1_ref, h1_ref, a2_ref, hid2_ref, dg2_ref, du2_ref, wg, wu, wd, turned_wd, sems):
    start = pl.program_id(0) == 0
    loads = [
        pltpu.make_async_copy(source, target, sems.at[i])
        for i, (source, target) in enumerate(
            (
                (wd_any.at[1], wd),
                (wg_any.at[0], wg.at[0]),
                (wu_any.at[0], wu.at[0]),
                (wg_any.at[1], wg.at[1]),
                (wu_any.at[1], wu.at[1]),
                (wd_any.at[0], wd),
            )
        )
    ]

    @pl.when(start)
    def _():
        for load in loads[:5]:
            load.start()
        loads[0].wait()
        turned(wd, turned_wd)
        loads[5].start()
        loads[1].wait()
        loads[2].wait()

    x = x_ref[...]
    a = normed(x)
    a1_ref[...] = a
    for c in range(0, wd.shape[0], CHUNK):
        at = slice(c, c + CHUNK)
        g, u = dot(a, wg[0, :, at]), dot(a, wu[0, :, at])
        g1_ref[:, at] = g
        u1_ref[:, at] = u
        hid1_ref[:, at] = narrow(g * jax.nn.sigmoid(g) * u)

    @pl.when(start)
    def _():
        loads[5].wait()
        loads[3].wait()
        loads[4].wait()

    h = narrow(x.astype(jnp.float32) + narrow(dot(hid1_ref[...], wd[...])).astype(jnp.float32))
    h1_ref[...] = h
    a = normed(h)
    a2_ref[...] = a
    dy = dy_ref[...]
    for c in range(0, wd.shape[0], CHUNK):
        at = slice(c, c + CHUNK)
        g, u = dot(a, wg[1, :, at]), dot(a, wu[1, :, at])
        hid, dg, du = through(g, u, dot(dy, turned_wd[:, at]))
        hid2_ref[:, at] = hid
        dg2_ref[:, at] = dg
        du2_ref[:, at] = du


def through(g, u, d):
    d = narrow(d).astype(jnp.float32)
    s = jax.nn.sigmoid(g)
    silu = g * s
    return narrow(silu * u), narrow(d * u * (s + silu * (1.0 - s))), narrow(d * silu)


def second_kernel(dy_ref, h1_ref, g1_ref, u1_ref, dg2_ref, du2_ref, wg_any, wu_any, wd_any, dh_ref, dg1_ref, du1_ref, wide, tall, turned_wg, turned_wu, turned_wd, sems):
    @pl.when(pl.program_id(0) == 0)
    def _():
        loads = [
            pltpu.make_async_copy(source, target, sems.at[i])
            for i, (source, target) in enumerate(((wg_any.at[1], wide.at[0]), (wu_any.at[1], wide.at[1]), (wd_any.at[0], tall)))
        ]
        for load in loads:
            load.start()
        for load, source, target in zip(loads, (wide.at[0], wide.at[1], tall), (turned_wg, turned_wu, turned_wd)):
            load.wait()
            turned(source, target)

    da = narrow(dot(dg2_ref[...], turned_wg[...])).astype(jnp.float32) + narrow(dot(du2_ref[...], turned_wu[...])).astype(jnp.float32)
    da = narrow(da).astype(jnp.float32)
    h = h1_ref[...].astype(jnp.float32)
    scale = lax.rsqrt(jnp.mean(h**2, -1, keepdims=True) + 1e-6)
    by_scale = jnp.sum(da * h, -1, keepdims=True)
    by_h = da * scale - h * (by_scale * scale * scale * scale / h.shape[1])
    dh = narrow(dy_ref[...].astype(jnp.float32) + narrow(by_h).astype(jnp.float32))
    dh_ref[...] = dh
    for c in range(0, tall.shape[0], CHUNK):
        at = slice(c, c + CHUNK)
        _, dg, du = through(g1_ref[:, at], u1_ref[:, at], dot(dh, turned_wd[:, at]))
        dg1_ref[:, at] = dg
        du1_ref[:, at] = du


def blocked(columns):
    return pl.BlockSpec((BLOCK, columns), lambda i: (i, 0))


def shaped(tokens, columns, dtype=jnp.bfloat16):
    return jax.ShapeDtypeStruct((tokens, columns), dtype)


HERE = pl.BlockSpec(memory_space=pl.ANY)
ALL_VMEM = pltpu.CompilerParams(vmem_limit_bytes=67_043_328, dimension_semantics=("arbitrary",))


def first_part(x, dy, w_gate, w_up, w_down):
    tokens, d = x.shape
    ff = w_down.shape[1]
    f32 = jnp.float32
    outs = [(d,), (ff, f32), (ff, f32), (ff,), (d,), (d,), (ff,), (ff,), (ff,)]
    return pl.pallas_call(
        first_kernel,
        grid=(tokens // BLOCK,),
        in_specs=[blocked(d)] * 2 + [HERE] * 3,
        out_specs=[blocked(o[0]) for o in outs],
        out_shape=[shaped(tokens, *o) for o in outs],
        scratch_shapes=[pltpu.VMEM((2, d, ff), jnp.bfloat16)] * 2 + [pltpu.VMEM((ff, d), jnp.bfloat16), pltpu.VMEM((d, ff), jnp.bfloat16), pltpu.SemaphoreType.DMA((6,))],
        compiler_params=ALL_VMEM,
        cost_estimate=pl.CostEstimate(flops=12 * tokens * d * ff, bytes_accessed=150_000_000, transcendentals=4 * tokens * ff),
        name="first_part",
    )(x, dy, w_gate, w_up, w_down)


def second_part(dy, h1, g1, u1, dg2, du2, w_gate, w_up, w_down):
    tokens, d = dy.shape
    ff = w_down.shape[1]
    bf16 = jnp.bfloat16
    return pl.pallas_call(
        second_kernel,
        grid=(tokens // BLOCK,),
        in_specs=[blocked(d)] * 2 + [blocked(ff)] * 4 + [HERE] * 3,
        out_specs=[blocked(d), blocked(ff), blocked(ff)],
        out_shape=[shaped(tokens, d), shaped(tokens, ff), shaped(tokens, ff)],
        scratch_shapes=[pltpu.VMEM((2, d, ff), bf16), pltpu.VMEM((ff, d), bf16)] + [pltpu.VMEM((ff, d), bf16)] * 2 + [pltpu.VMEM((d, ff), bf16), pltpu.SemaphoreType.DMA((3,))],
        compiler_params=ALL_VMEM,
        cost_estimate=pl.CostEstimate(flops=6 * tokens * d * ff, bytes_accessed=100_000_000, transcendentals=2 * tokens * ff),
        name="second_part",
    )(dy, h1, g1, u1, dg2, du2, w_gate, w_up, w_down)


def product(a, b):
    return narrow(lax.dot_general(a, b, (((0,), (0,)), ((), ())), preferred_element_type=jnp.float32))


def swap(array, bit):
    return lax.ppermute(array, "dp", [(i, i ^ bit) for i in range(DEVICES)])


def has(me, bit):
    return lax.shift_right_logical(me, jnp.int32(bit.bit_length() - 1)) & 1


def half_of(array, axis, which):
    size = array.shape[axis] // 2
    starts = [jnp.int32(0)] * array.ndim
    starts[axis] = which * size
    sizes = list(array.shape)
    sizes[axis] = size
    return lax.dynamic_slice(array, starts, sizes, allow_negative_indices=False)


def added(a, b):
    return narrow(a.astype(jnp.float32) + b.astype(jnp.float32))


class Scatter:
    def __init__(self, term, color, axes, me):
        self.parts, self.me = (term,), me
        self.left = list(zip((CORE, *XY[color], Z1, Z2), axes, strict=True))
        self.send()

    def piece(self, axis, which):
        parts = [half_of(part, axis, which) for part in self.parts]
        return parts[0] if len(parts) == 1 else added(*parts)

    def send(self):
        bit, axis = self.left.pop(0)
        mine = has(self.me, bit)
        out = self.piece(axis, 1 - mine)
        keep = self.piece(axis, mine)
        self.parts = (keep, swap(out, bit))
        self.sent = keep
        return keep

    def result(self):
        return added(*self.parts)


def gathered(shard, color, axes, me, behind):
    first, second = XY[color]
    held = shard
    for bit, axis in ((Z2, axes[4]), (Z1, axes[3])):
        got = swap(held, bit)
        mine = has(me, bit) == 1
        held = jnp.concatenate([jnp.where(mine, got, held), jnp.where(mine, held, got)], axis)
    got = swap(held, second)
    if behind:
        got = after(got, behind[0])
    held = jnp.concatenate([held, got], 0)
    other = swap(held, first)
    if behind:
        other = after(other, behind[1])
    return held, other, swap(held, CORE), swap(other, CORE)


def adamw_kernel(color, where_ref, factor_ref, w_ref, m_ref, v_ref, g0, g1, g2, g3, *rest):
    w_out, m_out, v_out, token = rest[-4:]
    token[...] = jnp.zeros_like(token)
    block = pl.program_id(0)
    outer, core = picked(color, block, where_ref)[:2]
    which = core * 2 + outer
    factor = factor_ref[0, 0]
    rows = w_ref.shape[1]
    step = 16
    for number, g_ref in enumerate((g0, g1, g2, g3)):

        @pl.when(which == number)
        def _():
            def some(i, _):
                at = pl.ds(pl.multiple_of(i * step, step), step)
                g = g_ref[at, :].astype(jnp.float32) * factor
                m = 0.9 * m_ref[0, at, :] + 0.1 * g
                v = 0.95 * v_ref[0, at, :] + 0.05 * g * g
                w = w_ref[0, at, :].astype(jnp.float32)
                w_out[0, at, :] = (w - 0.02 * (m * lax.rsqrt(v + 1e-8) + 0.1 * w)).astype(jnp.bfloat16)
                m_out[0, at, :] = m
                v_out[0, at, :] = v
                return 0

            lax.fori_loop(0, rows // step, some, 0)


def picked(color, block, where_ref):
    core, first, second = block // 4, (block // 2) % 2, block % 2
    return (first + where_ref[1]) % 2, (core + where_ref[0]) % 2, (second + where_ref[2]) % 2


def adamw(color, number, where, factor, w, m, v, pieces, so_far):
    layers, rows, columns = w.shape
    size = rows // 8
    whole = pl.BlockSpec((1, size, columns), lambda b, *_: (number, b, 0))

    def piece_at(which):
        def at(b, where_ref):
            outer, core, inner = picked(color, b, where_ref)
            return jnp.where(core * 2 + outer == which, inner, 0), 0

        return at

    out = [jax.ShapeDtypeStruct(w.shape, jnp.bfloat16)] + [jax.ShapeDtypeStruct(w.shape, jnp.float32)] * 2 + [jax.ShapeDtypeStruct((8, 128), jnp.float32)]
    old = list(so_far or ())
    return pl.pallas_call(
        functools.partial(adamw_kernel, color),
        out_shape=out,
        grid_spec=pltpu.PrefetchScalarGridSpec(
            num_scalar_prefetch=1,
            grid=(8,),
            in_specs=[pl.BlockSpec(memory_space=pltpu.SMEM)]
            + [whole] * 3
            + [pl.BlockSpec((size, columns), piece_at(which)) for which in range(4)]
            + [pl.BlockSpec(memory_space=pl.ANY)] * len(old),
            out_specs=[whole] * 3 + [pl.BlockSpec((8, 128), lambda b, *_: (0, 0))],
        ),
        input_output_aliases={9 + i: i for i in range(len(old))},
        compiler_params=pltpu.CompilerParams(vmem_limit_bytes=40 * 1024 * 1024),
        cost_estimate=pl.CostEstimate(flops=80_000_000, bytes_accessed=rows * columns * 22, transcendentals=rows * columns),
        name=f"adamw_{number}",
    )(where, factor, w, m, v, *pieces, *old)


AXES = {"w_gate": (0, 0, 0, 1, 1), "w_up": (0, 0, 0, 1, 1), "w_down": (0, 0, 0, 0, 0)}


def after(values, *first):
    return lax.optimization_barrier((values, first))[0]


def solution(mesh):
    def step(x, dy, *arrays):
        weights, m, v = (arrays[i : i + 3] for i in (0, 3, 6))
        layers = weights[0].shape[0]
        me = lax.axis_index("dp")
        color = {(name, number): (i + number) % 2 for i, name in enumerate(NAMES) for number in range(layers)}
        x, dy = x[0], dy[0]

        def scatter(name, number, a, b):
            return Scatter(product(a, b), color[name, number], AXES[name], me)

        def behind(done, *ones):
            for one in ones:
                one.parts = after(one.parts, done)

        a1, g1, u1, hid1, h1, a2, hid2, dg2, du2 = first_part(x, dy, *weights)
        d2 = scatter("w_down", 1, hid2, dy)
        g2 = scatter("w_gate", 1, *after((a2, dg2), d2.sent))
        behind(g2.sent, d2)
        u2 = scatter("w_up", 1, *after((a2, du2), g2.sent, d2.send()))
        behind(u2.sent, g2)
        dh1, dg1, du1 = second_part(*after((dy, h1, g1, u1, dg2, du2), g2.send(), u2.send()), *weights)
        behind(dh1, d2, g2, u2)
        d1 = scatter("w_down", 0, *after((hid1, dh1), d2.send(), u2.send()))
        behind(d1.sent, d2, g2, u2)
        g1_ = scatter("w_gate", 0, *after((a1, dg1), d1.sent, g2.send(), d2.send()))
        behind(g1_.sent, d2, g2, u2, d1)
        u1_ = scatter("w_up", 0, *after((a1, du1), g1_.sent, d1.send(), d2.send(), u2.send(), g2.send()))
        behind(u1_.sent, g1_, d1, u2, g2, d2)
        u1_.parts = after(u1_.parts, g1_.send(), g2.send(), u2.send())
        shards = {}
        second, first = (d2, g2, u2), (d1, g1_, u1_)
        shards = {}
        for name, one in zip(("w_down", "w_gate", "w_up"), second):
            assert not one.left
            shards[name, 1] = one.result()
        for name, one in zip(("w_down", "w_gate", "w_up"), first):
            while one.left:
                one.send()
            shards[name, 0] = one.result()
        squares = sum(jnp.sum(s.astype(jnp.float32) ** 2) for s in shards.values())
        count = sum(w.size for w in weights)
        factor = jnp.minimum(1.0, 0.5 * lax.rsqrt(lax.psum(squares, "dp") / count + 1e-30)).reshape(1, 1)
        new, order, tokens = {}, ("w_down", "w_gate", "w_up"), []
        wheres = [jnp.stack([has(me, bit) for bit in (CORE, *XY[c])]).astype(jnp.int32) for c in (0, 1)]
        for number in reversed(range(layers)):
            for name in order:
                i, c = NAMES.index(name), color[name, number]
                pieces = gathered(shards[name, number], c, AXES[name], me, tokens[:2] if number == 0 else [])
                *new[name], token = adamw(c, number, wheres[c], factor, weights[i], m[i], v[i], pieces, new.get(name))
                tokens.append(token)
        return tuple(new[name][which] for which in range(3) for name in NAMES)

    return jax.shard_map(
        step,
        mesh=mesh,
        in_specs=(P(("rep", "dp"), None, None),) * 2 + (P(None, None, None),) * 9,
        out_specs=(P("rep", None, None),) * 9,
        check_vma=False,
    )
```
